32 devices in a mesh: dp: 8 (over z, x), fsdp: 4 (over y, core).
Axes of the slice: x: 2, y: 2, z: 4, core: 2. Of those that a mesh axis runs over, the one named last changes fastest.
Arguments:
- hidden: bfloat16 [16, 256, 5120], P('dp', None, 'fsdp'), may hold values from -8 to 8
- gain: bfloat16 [5120], P('fsdp'), may hold values from 0.25 to 1.75
- head: bfloat16 [2048, 5120], P('fsdp'), may hold values from -1 to 1
- targets: int32 [16, 256], P('dp'), may hold values from 0 to 2047, as said below
- lengths: int32 [16], P('dp'), may hold values from 1 to 256, 2048 in all
- old_logp: float32 [16, 256], P('dp'), may hold values from -64 to 0
- rewards: float32 [16], P('dp'), may hold values from -6 to 6
- group_slot: int32 [16], P('dp'), may hold values from 0 to 15, each once
Outputs:
- loss: float32 [], replicated
- grad_hidden: bfloat16 [16, 256, 5120], P('dp', None, 'fsdp')
- grad_gain: float32 [5120], P('fsdp')
- grad_head_t: float32 [5120, 2048], P('dp', 'fsdp')
The draws below stay inside these ranges and needn't reach their ends.
Inputs may be any that keep to these rules, and one draw needn't show every extreme that they name: `lengths`: they sum to 2048 and one of them equals 256. `group_slot`: each value once; responses with equal group_slot // 8 answer one prompt. At position 0, different responses have different targets.
All inputs are finite; a program needn't handle non-finite values. No bound on the sum of `lengths` on one device may be relied on, other than what follows from the above.
Results may differ from the reference program's by a relative error of at most 0.018.
Values may be sent and summed in bfloat16 or wider, within the bound.
A program may use at most 64 MiB of HBM per device.

```python
import math
import jax
import jax.numpy as jnp
import numpy as np
from jax import lax

D = 5120
VOC_DEV = 512
LEN = 256
GROUP = 8
RESP_DEV = 2
RESPONSES = 16
VOCAB = 2048
NGROUPS = 2
TOKENS = 4096
N_DP = 8
N_FSDP = 4


def drawn_entries(key):
    amount = RESPONSES
    order = jax.random.permutation(jax.random.fold_in(key, 7001), VOCAB).astype(jnp.int32)
    return order[:amount]


def draw_targets(key, part):
    upper_ids = drawn_entries(key)
    base = jax.random.randint(jax.random.fold_in(key, 7101), (RESPONSES, LEN), 0, VOCAB, jnp.int32)
    return base.at[:, 0].set(upper_ids)


def draw_hidden(key, part):
    base = jax.random.normal(jax.random.fold_in(key, 7201), (RESPONSES, LEN, D), jnp.float32)
    base = jnp.clip(base, -6.0, 6.0)
    return base.astype(jnp.bfloat16)


def draw_gain(key, part):
    base = jax.random.normal(jax.random.fold_in(key, 7501), (D,), jnp.float32)
    return (1.0 + 0.15 * jnp.clip(base, -5.0, 5.0)).astype(jnp.bfloat16)


def draw_head(key, part):
    spread = math.sqrt(9.0 / D)
    base = jax.random.normal(jax.random.fold_in(key, 7301), (VOCAB, D), jnp.float32) * spread
    base = jnp.clip(base, -6.0 * spread, 6.0 * spread)
    return base.astype(jnp.bfloat16)


def draw_old_logp(key, part):
    states = draw_hidden(key, part)
    gain_f = draw_gain(key, part).astype(jnp.float32)
    weights = draw_head(key, part)
    picks = draw_targets(key, part)

    def response_logp(item):
        rows_here, chosen_ids = item
        values = rows_here.astype(jnp.float32)
        inv = lax.rsqrt(jnp.mean(values * values, axis=1, keepdims=True) + 1e-06)
        normed = (values * inv * gain_f).astype(jnp.bfloat16)
        logits = lax.dot_general(normed, weights, (((1,), (1,)), ((), ())), preferred_element_type=jnp.float32)
        top = jnp.max(logits, axis=1)
        lse = top + jnp.log(jnp.sum(jnp.exp(logits - top[:, None]), axis=1))
        hits = jnp.arange(VOCAB, dtype=jnp.int32)[None, :] == chosen_ids[:, None]
        return jnp.sum(jnp.where(hits, logits, 0.0), axis=1) - lse
    logp = lax.map(response_logp, (states, picks))
    band = jax.random.randint(jax.random.fold_in(key, 7402), (RESPONSES, LEN), 0, 4, jnp.int32)
    lows = jnp.log(jnp.array([0.5, 0.88, 1.4, 3.6], jnp.float32))
    highs = jnp.log(jnp.array([0.7, 1.12, 2.5, 6.0], jnp.float32))
    lower_edge = jnp.take(lows, band)
    upper_edge = jnp.take(highs, band)
    level = jax.random.uniform(jax.random.fold_in(key, 7403), (RESPONSES, LEN), jnp.float32, 0.0, 1.0)
    logratio = lower_edge + level * (upper_edge - lower_edge)
    older = logp - logratio
    older = jnp.where(older > 0.0, logp - math.log(2.0), older)
    return jnp.clip(older, -64.0, 0.0)


def block_scale(key, dims, split, smallest, high):
    level = 1.0
    for axis_at, shards_of in split:
        heights = jax.random.uniform(jax.random.fold_in(jax.random.fold_in(key, 6), axis_at), (shards_of,), jnp.float32, smallest / len(split), high / len(split))
        level = level * jnp.repeat(jnp.exp(heights), dims[axis_at] // shards_of).reshape((-1,) + (1,) * (len(dims) - 1 - axis_at))
    return level


def length_profile(number_of, total, limit, lean):
    loads = [(1 << 20) // math.isqrt(standing ** lean) + 1 for standing in range(2, number_of + 1)]
    surplus, counts = total - limit - (number_of - 1), [1] * (number_of - 1)
    while surplus > 0:
        candidates = [i for i in range(number_of - 1) if counts[i] < limit]
        pool, budget = sum([loads[i] for i in candidates]), surplus
        for i in candidates:
            more = min(limit - counts[i], max(1, budget * loads[i] // pool), surplus)
            counts[i] = counts[i] + more
            surplus = surplus - more
    return np.array([limit] + counts)


def uneven(own_key, count, total, limit, skew):
    if count == 2:
        one = jax.random.randint(own_key, (), max(1, total - limit), min(limit, total - 1) + 1)
        return jnp.stack([one, total - one])
    sizes = jnp.asarray(length_profile(count, total, limit, skew), jnp.int32)
    couples = (count - 1) // 2
    source_of, taker = sizes[1:1 + 2 * couples:2], sizes[2:2 + 2 * couples:2]
    slack = jnp.minimum(source_of - 1, limit - taker)
    shifted = jax.random.randint(jax.random.fold_in(own_key, 1), (couples,), 0, 1 << 20) % (slack + 1)
    sizes = sizes.at[1:1 + 2 * couples:2].set(source_of - shifted).at[2:2 + 2 * couples:2].set(taker + shifted)
    return sizes[jax.random.permutation(jax.random.fold_in(own_key, 2), count)]


def normal_values(own_key, shape, scale, reach, split=(), kind=jnp.bfloat16):
    result = scale * jax.random.normal(own_key, shape, jnp.float32)
    if split:
        result = result * block_scale(own_key, shape, split, -0.22, 0.18)
    return jnp.clip(result, -reach, reach).astype(kind)


def setup_inputs(seed: int = 0) -> dict:
    key_list = jax.random.split(jax.random.key(seed), 9)
    hidden = draw_hidden(jax.random.fold_in(key_list[8], 71), 0)
    gain = draw_gain(jax.random.fold_in(key_list[8], 71), 0)
    head = draw_head(jax.random.fold_in(key_list[8], 71), 0)
    targets = draw_targets(jax.random.fold_in(key_list[8], 71), 0)
    lengths = uneven(key_list[4], RESPONSES, RESPONSES * LEN // 2, LEN, 2).astype(jnp.int32)
    old_logp = draw_old_logp(jax.random.fold_in(key_list[8], 71), 0)
    rewards = normal_values(key_list[6], (RESPONSES,), 1.0, 6.0, ((0, 8),), jnp.float32)
    group_slot = jax.random.permutation(key_list[7], RESPONSES).astype(jnp.int32)
    return {"hidden": hidden, "gain": gain, "head": head, "targets": targets, "lengths": lengths, "old_logp": old_logp, "rewards": rewards, "group_slot": group_slot}


eps_norm = 1e-06
clip_low = 0.8
clip_high = 1.2
dual_bound = 3.0

def reference(hidden, gain, head, targets, lengths, old_logp, rewards, group_slot):
    rows = RESPONSES * LEN
    h = hidden.reshape(rows, D).astype(jnp.float32)
    inv = lax.rsqrt(lax.optimization_barrier(jnp.mean(h * h, axis=1, keepdims=True)) + eps_norm)
    gain_f = gain.astype(jnp.float32)
    normed = (h * inv * gain_f).astype(jnp.bfloat16)
    logits = lax.dot_general(normed.astype(jnp.float32), head.astype(jnp.float32), (((1,), (1,)), ((), ())), preferred_element_type=jnp.float32)
    top = lax.optimization_barrier(jnp.max(logits, axis=1, keepdims=True))
    lse = top[:, 0] + jnp.log(lax.optimization_barrier(jnp.sum(jnp.exp(logits - top), axis=1)))
    flat_targets = targets.reshape(rows).astype(jnp.int32)
    hits = jnp.arange(VOCAB, dtype=jnp.int32)[None, :] == flat_targets[:, None]
    chosen = lax.optimization_barrier(jnp.sum(jnp.where(hits, logits, 0.0), axis=1))
    logp = chosen - lse
    group = group_slot // GROUP
    member = (group[:, None] == jnp.arange(NGROUPS, dtype=jnp.int32)[None, :]).astype(jnp.float32)
    group_sums = lax.optimization_barrier(jnp.sum(member * rewards[:, None], axis=0))
    adv_resp = rewards - lax.optimization_barrier(jnp.sum(member * group_sums[None, :], axis=1)) / GROUP
    adv = jnp.repeat(adv_resp, LEN)
    mask = (jnp.arange(LEN, dtype=jnp.int32)[None, :] < lengths[:, None]).astype(jnp.float32).reshape(rows)
    count = jnp.sum(lengths).astype(jnp.float32)
    ratio = jnp.exp(logp - old_logp.reshape(rows))
    first = ratio * adv
    second = jnp.clip(ratio, clip_low, clip_high) * adv
    policy = -jnp.minimum(first, second)
    policy = jnp.where(adv < 0, jnp.minimum(policy, -dual_bound * adv), policy)
    loss = jnp.sum(mask * policy) / count
    active = (first <= second) & jnp.logical_not((adv < 0) & (first < dual_bound * adv))
    grad_logp = TOKENS / count * mask * jnp.where(active, -ratio * adv, 0.0)
    probs = jnp.exp(logits - lse[:, None])
    dlogits = (grad_logp[:, None] * (hits.astype(jnp.float32) - probs)).astype(jnp.bfloat16)

    def add_block(total, index):
        piece = lax.dynamic_slice_in_dim(dlogits, index * VOC_DEV, VOC_DEV, 1)
        rows_w = lax.dynamic_slice_in_dim(head, index * VOC_DEV, VOC_DEV, 0)
        term = jnp.dot(piece.astype(jnp.float32), rows_w.astype(jnp.float32), preferred_element_type=jnp.float32)
        return (total + term.astype(jnp.bfloat16).astype(jnp.float32), None)
    dnormed, _ = lax.scan(add_block, jnp.zeros((rows, D), jnp.float32), jnp.arange(N_FSDP, dtype=jnp.int32))
    dy = dnormed * gain_f
    dots = lax.optimization_barrier(jnp.sum(h * dy, axis=1, keepdims=True))
    grad_h = inv * dy - h * inv * inv * inv * dots / D
    grad_hidden = grad_h.astype(jnp.bfloat16).reshape(RESPONSES, LEN, D)
    grad_gain = lax.optimization_barrier(jnp.sum(dnormed * h * inv, axis=0))
    per_group = RESP_DEV * LEN

    def add_group(total, index):
        left = lax.dynamic_slice_in_dim(normed, index * per_group, per_group, 0)
        right = lax.dynamic_slice_in_dim(dlogits, index * per_group, per_group, 0)
        term = lax.dot_general(left.astype(jnp.float32), right.astype(jnp.float32), (((0,), (0,)), ((), ())), preferred_element_type=jnp.float32)
        return (total + term.astype(jnp.bfloat16).astype(jnp.float32), None)
    grad_head_t, _ = lax.scan(add_group, jnp.zeros((D, VOCAB), jnp.float32), jnp.arange(N_DP, dtype=jnp.int32))
    return (loss, grad_hidden, grad_gain, grad_head_t)
```

```python
import functools
import jax
import jax.numpy as jnp
from jax import lax
from jax.experimental import pallas as pl
from jax.experimental.pallas import tpu as pltpu
from jax.sharding import PartitionSpec as P

GROUP = 8


eps_norm = 1e-06
clip_low = 0.8
clip_high = 1.2
dual_bound = 3.0


MESH = pl.DeviceIdType.MESH


def tail_kernel(
    n_dp,
    n_fsdp,
    feats,
    normed_ref,
    dlogits_ref,
    head_ref,
    hidden_ref,
    gain_ref,
    inv_ref,
    loss_ref,
    gh_ref,
    gw_ref,
    gg_ref,
    x_out,
    x_in,
    z_out,
    z_in,
    c_out,
    c_in,
    y_out,
    y_in,
    acc,
    d_out,
    d_in,
    g_out,
    g_in,
    xs,
    xr,
    zs,
    zr,
    cs,
    cr,
    ys,
    yr,
    ds_,
    dr,
    gs,
    gr,
):
    dp = lax.axis_index("dp")
    fs = lax.axis_index("fsdp")
    z, x = dp // 2, dp % 2
    y, c = fs // 2, fs % 2
    outer_dp, outer_fs = n_dp // 2, n_fsdp // 2
    cols = hidden_ref.shape[1]

    barrier = pltpu.get_barrier_semaphore()
    for k in range(1, n_dp):
        pl.semaphore_signal(barrier, inc=1, device_id=(dp ^ k, fs), device_id_type=MESH)
    for k in range(1, n_fsdp):
        pl.semaphore_signal(barrier, inc=1, device_id=(dp, fs ^ k), device_id_type=MESH)
    pl.semaphore_wait(barrier, n_dp + n_fsdp - 2)

    def remote(out, into, send, recv, k, dst):
        return pltpu.make_async_remote_copy(
            src_ref=out,
            dst_ref=into.at[k],
            send_sem=send.at[k],
            recv_sem=recv.at[k],
            device_id=dst,
            device_id_type=MESH,
        )

    def x_copy(k):
        return remote(x_out.at[k], x_in, xs, xr, k, (dp ^ 1, fs))

    def z_copy(k):
        return remote(z_out.at[k], z_in, zs, zr, k, ((z ^ k) * 2 + x, fs))

    def c_copy(j):
        return remote(c_out.at[j], c_in, cs, cr, j, (dp, fs ^ 1))

    def y_copy(j):
        return remote(y_out.at[j], y_in, ys, yr, j, (dp, (y ^ j) * 2 + c))

    def d_copy(j):
        return remote(d_out, d_in, ds_, dr, j, (dp, fs ^ j))

    def g_copy(k):
        return remote(g_out, g_in, gs, gr, k, (dp ^ k, fs))

    def dw(block):
        if feats % 128 == 0:
            left = normed_ref[:, pl.ds(pl.multiple_of(block * feats, 128), feats)]
        else:
            left = normed_ref[block]
        return lax.dot_general(
            left, dlogits_ref[...], (((0,), (0,)), ((), ())), preferred_element_type=jnp.float32
        )

    def dn(block):
        right = head_ref[:, pl.ds(pl.multiple_of(block * cols, 128), cols)]
        return jnp.dot(dlogits_ref[...], right, preferred_element_type=jnp.float32)

    @pl.loop(0, outer_dp)
    def _(i):
        k = outer_dp - 1 - i
        x_out[k] = dw((z ^ k) * 2 + (1 - x)).astype(jnp.bfloat16)
        x_copy(k).start()

    @pl.loop(0, outer_fs)
    def _(i):
        j = outer_fs - 1 - i
        c_out[j] = dn((y ^ j) * 2 + (1 - c)).astype(jnp.bfloat16)
        c_copy(j).start()

    @pl.loop(0, outer_fs - 1)
    def _(i):
        j = outer_fs - 1 - i
        mine = dn((y ^ j) * 2 + c)
        c_copy(j).wait_recv()
        y_out[j] = (mine + c_in[j].astype(jnp.float32)).astype(jnp.bfloat16)
        y_copy(j).start()

    acc[...] = dn(fs)
    c_copy(0).wait_recv()
    acc[...] += c_in[0].astype(jnp.float32)

    @pl.loop(0, outer_dp - 1)
    def _(i):
        k = outer_dp - 1 - i
        mine = dw((z ^ k) * 2 + x)
        x_copy(k).wait_recv()
        z_out[k] = (mine + x_in[k].astype(jnp.float32)).astype(jnp.bfloat16)
        z_copy(k).start()

    @pl.loop(1, outer_fs)
    def _(j):
        y_copy(j).wait_recv()
        acc[...] += y_in[j].astype(jnp.float32)

    h = hidden_ref[...].astype(jnp.float32)
    inv = inv_ref[...]
    g_out[:, :cols] = jnp.broadcast_to(
        jnp.sum(acc[...] * h * inv, axis=0, keepdims=True), (8, cols)
    )
    g_out[:, cols:] = loss_ref[...]

    @pl.loop(1, n_dp)
    def _(k):
        g_copy(k).start()

    dy = acc[...] * gain_ref[...]
    part = jnp.sum(h * dy, axis=1, keepdims=True)
    rows = part.shape[0]
    d_out[...] = jnp.transpose(jnp.broadcast_to(part, (rows, 128)))[:8]
    for j in range(1, n_fsdp):
        d_copy(j).start()
    dots = d_out[...]
    for j in range(1, n_fsdp):
        d_copy(j).wait_recv()
        dots += d_in[j]
    column = jnp.transpose(jnp.broadcast_to(dots[:1], (128, rows)))[:, :1]
    scale = inv * inv * inv * column / (cols * n_fsdp)
    gh_ref[...] = (
        inv * (acc[...] * gain_ref[...]) - hidden_ref[...].astype(jnp.float32) * scale
    ).astype(jnp.bfloat16)

    gg_ref[...] = g_out[...]

    @pl.loop(1, n_dp)
    def _(k):
        g_copy(k).wait_recv()
        gg_ref[...] += g_in[k]

    own = dw(dp)
    x_copy(0).wait_recv()
    gw_ref[...] = own + x_in[0].astype(jnp.float32)

    @pl.loop(0, outer_dp - 1)
    def _(i):
        k = outer_dp - 1 - i
        z_copy(k).wait_recv()
        gw_ref[...] += z_in[k].astype(jnp.float32)

    @pl.loop(0, outer_dp)
    def _(k):
        x_copy(k).wait_send()

    @pl.loop(1, outer_dp)
    def _(k):
        z_copy(k).wait_send()

    @pl.loop(0, outer_fs)
    def _(j):
        c_copy(j).wait_send()

    @pl.loop(1, outer_fs)
    def _(j):
        y_copy(j).wait_send()

    for j in range(1, n_fsdp):
        d_copy(j).wait_send()

    @pl.loop(1, n_dp)
    def _(k):
        g_copy(k).wait_send()


def tail(normed, dlogits, head, hidden, gain_row, inv, loss_tile):
    n_dp, n_fsdp = lax.axis_size("dp"), lax.axis_size("fsdp")
    rows, width = normed.shape
    vocab_here = head.shape[0]
    cols = hidden.shape[1]
    feats = width // n_dp
    zd, yd = n_dp // 2, n_fsdp // 2
    if feats % 128:
        normed = normed.reshape(rows, n_dp, feats).transpose(1, 0, 2)
    wide = cols + 128
    bf, f32 = jnp.bfloat16, jnp.float32
    vm = pl.BlockSpec(memory_space=pltpu.VMEM)
    dma = pltpu.SemaphoreType.DMA
    return pl.pallas_call(
        functools.partial(tail_kernel, n_dp, n_fsdp, feats),
        out_shape=(
            jax.ShapeDtypeStruct((rows, cols), bf),
            jax.ShapeDtypeStruct((feats, vocab_here), f32),
            jax.ShapeDtypeStruct((8, wide), f32),
        ),
        in_specs=[vm] * 7,
        out_specs=(vm, vm, vm),
        scratch_shapes=[
            pltpu.VMEM((zd, feats, vocab_here), bf),
            pltpu.VMEM((zd, feats, vocab_here), bf),
            pltpu.VMEM((zd, feats, vocab_here), bf),
            pltpu.VMEM((zd, feats, vocab_here), bf),
            pltpu.VMEM((yd, rows, cols), bf),
            pltpu.VMEM((yd, rows, cols), bf),
            pltpu.VMEM((yd, rows, cols), bf),
            pltpu.VMEM((yd, rows, cols), bf),
            pltpu.VMEM((rows, cols), f32),
            pltpu.VMEM((8, rows), f32),
            pltpu.VMEM((n_fsdp, 8, rows), f32),
            pltpu.VMEM((8, wide), f32),
            pltpu.VMEM((n_dp, 8, wide), f32),
        ]
        + [dma((n,)) for n in (zd, zd, zd, zd, yd, yd, yd, yd, n_fsdp, n_fsdp, n_dp, n_dp)],
        compiler_params=pltpu.CompilerParams(
            collective_id=0, has_side_effects=True, vmem_limit_bytes=60 * 1024 * 1024
        ),
    )(normed, dlogits, head, hidden, gain_row, inv, loss_tile)


def body(hidden, gain, head, targets, lengths, old_logp, rewards, group_slot):
    resp_here, length_max, shard_cols = hidden.shape
    rows = resp_here * length_max
    whole, gain_full = (
        lax.all_gather(hidden, "fsdp", axis=2, tiled=True),
        lax.all_gather(gain, "fsdp", axis=0, tiled=True),
    )
    width = whole.shape[2]
    whole = whole.reshape(rows, width)
    vocab_here = head.shape[0]
    vocab_start = lax.axis_index("fsdp") * vocab_here
    groups_all = resp_here * lax.axis_size("dp") // GROUP
    group = group_slot // GROUP
    member = (group[:, None] == jnp.arange(groups_all, dtype=jnp.int32)[None, :]).astype(
        jnp.float32
    )
    local_sums = jnp.sum(member * rewards[:, None], axis=0)
    local_count = jnp.sum(lengths).astype(jnp.float32)
    group_sums, count = lax.psum((local_sums, local_count), "dp")
    adv_resp = rewards - jnp.sum(member * group_sums[None, :], axis=1) / GROUP
    adv = jnp.repeat(adv_resp, length_max)
    mask = (
        (jnp.arange(length_max, dtype=jnp.int32)[None, :] < lengths[:, None])
        .astype(jnp.float32)
        .reshape(rows)
    )
    gain_f = gain_full.astype(jnp.float32)
    inv = lax.rsqrt(
        jnp.mean(jnp.square(whole.astype(jnp.float32)), axis=1, keepdims=True) + eps_norm
    )
    normed = (whole.astype(jnp.float32) * inv * gain_f).astype(jnp.bfloat16)
    logits = lax.dot_general(
        normed, head, (((1,), (1,)), ((), ())), preferred_element_type=jnp.float32
    )
    top_local = jnp.max(logits, axis=1)
    sum_local = jnp.sum(jnp.exp(logits - top_local[:, None]), axis=1)
    local_targets = targets.reshape(rows) - vocab_start
    hits = jnp.arange(vocab_here, dtype=jnp.int32)[None, :] == local_targets[:, None]
    chosen_local = jnp.sum(jnp.where(hits, logits, 0.0), axis=1)
    stats = lax.all_gather(jnp.stack([top_local, sum_local, chosen_local]), "fsdp", axis=0)
    top = jnp.max(stats[:, 0], axis=0)
    total = jnp.sum(stats[:, 1] * jnp.exp(stats[:, 0] - top[None, :]), axis=0)
    chosen = jnp.sum(stats[:, 2], axis=0)
    lse = top + jnp.log(total)
    logp = chosen - lse
    ratio = jnp.exp(logp - old_logp.reshape(rows))
    first = ratio * adv
    second = jnp.clip(ratio, clip_low, clip_high) * adv
    policy = -jnp.minimum(first, second)
    policy = jnp.where(adv < 0, jnp.minimum(policy, -dual_bound * adv), policy)
    loss_local = jnp.sum(mask * policy)
    active = (first <= second) & jnp.logical_not((adv < 0) & (first < dual_bound * adv))
    slots_all = rows * lax.axis_size("dp")
    grad_logp = slots_all / count * mask * jnp.where(active, -ratio * adv, 0.0)
    probs = jnp.exp(logits - lse[:, None])
    dlogits = (grad_logp[:, None] * (hits.astype(jnp.float32) - probs)).astype(jnp.bfloat16)
    grad_h, grad_head_t, sums = tail(
        normed,
        dlogits,
        head,
        hidden.reshape(rows, shard_cols),
        gain.astype(jnp.float32)[None, :],
        inv,
        jnp.broadcast_to(loss_local, (8, 128)),
    )
    loss = sums[0, shard_cols] / count
    grad_gain = sums[0, :shard_cols]
    grad_hidden = grad_h.reshape(resp_here, length_max, shard_cols)
    return (loss, grad_hidden, grad_gain, grad_head_t)


def solution(mesh):
    in_specs = (
        P("dp", None, "fsdp"),
        P("fsdp"),
        P("fsdp", None),
        P("dp", None),
        P("dp"),
        P("dp", None),
        P("dp"),
        P("dp"),
    )
    out_specs = (P(), P("dp", None, "fsdp"), P("fsdp"), P("dp", "fsdp"))
    return jax.shard_map(body, mesh=mesh, in_specs=in_specs, out_specs=out_specs, check_vma=False)
```

```python
import functools
import jax
import jax.numpy as jnp
from jax import lax
from jax.experimental import pallas as pl
from jax.experimental.pallas import tpu as pltpu
from jax.sharding import PartitionSpec as P

GROUP = 8


eps_norm = 1e-06
clip_low = 0.8
clip_high = 1.2
dual_bound = 3.0


MESH = pl.DeviceIdType.MESH


def tail_kernel(
    n_dp,
    n_fsdp,
    feats,
    normed_ref,
    dlogits_ref,
    head_ref,
    hidden_ref,
    gain_ref,
    inv_ref,
    loss_ref,
    gh_ref,
    gw_ref,
    gg_ref,
    x_out,
    x_in,
    n_out,
    n_in,
    z_out,
    z_in,
    c_out,
    c_in,
    y_out,
    y_in,
    acc,
    d_out,
    d_in,
    g_out,
    g_in,
    xs,
    xr,
    ns,
    nr,
    zs,
    zr,
    cs,
    cr,
    ys,
    yr,
    ds_,
    dr,
    gs,
    gr,
):
    dp = lax.axis_index("dp")
    fs = lax.axis_index("fsdp")
    z, x = dp // 2, dp % 2
    y, c = fs // 2, fs % 2
    outer_dp, outer_fs, quads = n_dp // 2, n_fsdp // 2, n_dp // 4
    cols = hidden_ref.shape[1]

    barrier = pltpu.get_barrier_semaphore()
    for k in range(1, n_dp):
        pl.semaphore_signal(barrier, inc=1, device_id=(dp ^ k, fs), device_id_type=MESH)
    for k in range(1, n_fsdp):
        pl.semaphore_signal(barrier, inc=1, device_id=(dp, fs ^ k), device_id_type=MESH)
    pl.semaphore_wait(barrier, n_dp + n_fsdp - 2)

    def remote(out, into, send, recv, k, dst):
        return pltpu.make_async_remote_copy(
            src_ref=out,
            dst_ref=into.at[k],
            send_sem=send.at[k],
            recv_sem=recv.at[k],
            device_id=dst,
            device_id_type=MESH,
        )

    def x_copy(k):
        return remote(x_out.at[k], x_in, xs, xr, k, (dp ^ 1, fs))

    def z_copy(k):
        return remote(z_out.at[k], z_in, zs, zr, k, (dp ^ (4 * k), fs))

    def n_copy(k):
        return remote(n_out.at[k], n_in, ns, nr, k, (dp ^ 2, fs))

    def c_copy(j):
        return remote(c_out.at[j], c_in, cs, cr, j, (dp, fs ^ 1))

    def y_copy(j):
        return remote(y_out.at[j], y_in, ys, yr, j, (dp, (y ^ j) * 2 + c))

    def d_copy(j):
        return remote(d_out, d_in, ds_, dr, j, (dp, fs ^ j))

    def g_copy(k):
        return remote(g_out, g_in, gs, gr, k, (dp ^ k, fs))

    def dw(block):
        if feats % 128 == 0:
            left = normed_ref[:, pl.ds(pl.multiple_of(block * feats, 128), feats)]
        else:
            left = normed_ref[block]
        return lax.dot_general(
            left, dlogits_ref[...], (((0,), (0,)), ((), ())), preferred_element_type=jnp.float32
        )

    def dn(block):
        right = head_ref[:, pl.ds(pl.multiple_of(block * cols, 128), cols)]
        return jnp.dot(dlogits_ref[...], right, preferred_element_type=jnp.float32)

    @pl.loop(0, outer_dp)
    def _(i):
        k = outer_dp - 1 - i
        x_out[k] = dw((z ^ k) * 2 + (1 - x)).astype(jnp.bfloat16)
        x_copy(k).start()

    @pl.loop(0, outer_fs)
    def _(i):
        j = outer_fs - 1 - i
        c_out[j] = dn((y ^ j) * 2 + (1 - c)).astype(jnp.bfloat16)
        c_copy(j).start()

    @pl.loop(0, outer_fs - 1)
    def _(i):
        j = outer_fs - 1 - i
        mine = dn((y ^ j) * 2 + c)
        c_copy(j).wait_recv()
        y_out[j] = (mine + c_in[j].astype(jnp.float32)).astype(jnp.bfloat16)
        y_copy(j).start()

    acc[...] = dn(fs)
    c_copy(0).wait_recv()
    acc[...] += c_in[0].astype(jnp.float32)

    def pair_sum(k):
        mine = dw((z ^ k) * 2 + x)
        x_copy(k).wait_recv()
        return mine + x_in[k].astype(jnp.float32)

    def to_near(q):
        n_out[q] = pair_sum(2 * q + 1).astype(jnp.bfloat16)
        n_copy(q).start()

    @pl.loop(0, quads - 1)
    def _(i):
        q = quads - 1 - i
        to_near(q)
        mine = pair_sum(2 * q)
        n_copy(q).wait_recv()
        z_out[q] = (mine + n_in[q].astype(jnp.float32)).astype(jnp.bfloat16)
        z_copy(q).start()

    to_near(0)

    @pl.loop(1, outer_fs)
    def _(j):
        y_copy(j).wait_recv()
        acc[...] += y_in[j].astype(jnp.float32)

    h = hidden_ref[...].astype(jnp.float32)
    inv = inv_ref[...]
    g_out[:, :cols] = jnp.broadcast_to(
        jnp.sum(acc[...] * h * inv, axis=0, keepdims=True), (8, cols)
    )
    g_out[:, cols:] = loss_ref[...]

    @pl.loop(1, n_dp)
    def _(k):
        g_copy(k).start()

    dy = acc[...] * gain_ref[...]
    part = jnp.sum(h * dy, axis=1, keepdims=True)
    rows = part.shape[0]
    d_out[...] = jnp.transpose(jnp.broadcast_to(part, (rows, 128)))[:8]
    for j in range(1, n_fsdp):
        d_copy(j).start()
    dots = d_out[...]
    for j in range(1, n_fsdp):
        d_copy(j).wait_recv()
        dots += d_in[j]
    column = jnp.transpose(jnp.broadcast_to(dots[:1], (128, rows)))[:, :1]
    scale = inv * inv * inv * column / (cols * n_fsdp)
    gh_ref[...] = (
        inv * (acc[...] * gain_ref[...]) - hidden_ref[...].astype(jnp.float32) * scale
    ).astype(jnp.bfloat16)

    gg_ref[...] = g_out[...]

    @pl.loop(1, n_dp)
    def _(k):
        g_copy(k).wait_recv()
        gg_ref[...] += g_in[k]

    gw_ref[...] = pair_sum(0)
    n_copy(0).wait_recv()
    gw_ref[...] += n_in[0].astype(jnp.float32)

    @pl.loop(1, quads)
    def _(k):
        z_copy(k).wait_recv()
        gw_ref[...] += z_in[k].astype(jnp.float32)

    @pl.loop(0, outer_dp)
    def _(k):
        x_copy(k).wait_send()

    @pl.loop(0, quads)
    def _(k):
        n_copy(k).wait_send()

    @pl.loop(1, quads)
    def _(k):
        z_copy(k).wait_send()

    @pl.loop(0, outer_fs)
    def _(j):
        c_copy(j).wait_send()

    @pl.loop(1, outer_fs)
    def _(j):
        y_copy(j).wait_send()

    for j in range(1, n_fsdp):
        d_copy(j).wait_send()

    @pl.loop(1, n_dp)
    def _(k):
        g_copy(k).wait_send()


def tail(normed, dlogits, head, hidden, gain_row, inv, loss_tile):
    n_dp, n_fsdp = lax.axis_size("dp"), lax.axis_size("fsdp")
    rows, width = normed.shape
    vocab_here = head.shape[0]
    cols = hidden.shape[1]
    feats = width // n_dp
    zd, qd, yd = n_dp // 2, n_dp // 4, n_fsdp // 2
    if feats % 128:
        normed = normed.reshape(rows, n_dp, feats).transpose(1, 0, 2)
    wide = cols + 128
    bf, f32 = jnp.bfloat16, jnp.float32
    vm = pl.BlockSpec(memory_space=pltpu.VMEM)
    dma = pltpu.SemaphoreType.DMA
    return pl.pallas_call(
        functools.partial(tail_kernel, n_dp, n_fsdp, feats),
        out_shape=(
            jax.ShapeDtypeStruct((rows, cols), bf),
            jax.ShapeDtypeStruct((feats, vocab_here), f32),
            jax.ShapeDtypeStruct((8, wide), f32),
        ),
        in_specs=[vm] * 7,
        out_specs=(vm, vm, vm),
        scratch_shapes=[
            pltpu.VMEM((zd, feats, vocab_here), bf),
            pltpu.VMEM((zd, feats, vocab_here), bf),
            pltpu.VMEM((qd, feats, vocab_here), bf),
            pltpu.VMEM((qd, feats, vocab_here), bf),
            pltpu.VMEM((qd, feats, vocab_here), bf),
            pltpu.VMEM((qd, feats, vocab_here), bf),
            pltpu.VMEM((yd, rows, cols), bf),
            pltpu.VMEM((yd, rows, cols), bf),
            pltpu.VMEM((yd, rows, cols), bf),
            pltpu.VMEM((yd, rows, cols), bf),
            pltpu.VMEM((rows, cols), f32),
            pltpu.VMEM((8, rows), f32),
            pltpu.VMEM((n_fsdp, 8, rows), f32),
            pltpu.VMEM((8, wide), f32),
            pltpu.VMEM((n_dp, 8, wide), f32),
        ]
        + [dma((n,)) for n in (zd, zd, qd, qd, qd, qd, yd, yd, yd, yd, n_fsdp, n_fsdp, n_dp, n_dp)],
        compiler_params=pltpu.CompilerParams(
            collective_id=0, has_side_effects=True, vmem_limit_bytes=60 * 1024 * 1024
        ),
    )(normed, dlogits, head, hidden, gain_row, inv, loss_tile)


def body(hidden, gain, head, targets, lengths, old_logp, rewards, group_slot):
    resp_here, length_max, shard_cols = hidden.shape
    rows = resp_here * length_max
    whole, gain_full = (
        lax.all_gather(hidden, "fsdp", axis=2, tiled=True),
        lax.all_gather(gain, "fsdp", axis=0, tiled=True),
    )
    width = whole.shape[2]
    whole = whole.reshape(rows, width)
    vocab_here = head.shape[0]
    vocab_start = lax.axis_index("fsdp") * vocab_here
    groups_all = resp_here * lax.axis_size("dp") // GROUP
    group = group_slot // GROUP
    member = (group[:, None] == jnp.arange(groups_all, dtype=jnp.int32)[None, :]).astype(
        jnp.float32
    )
    local_sums = jnp.sum(member * rewards[:, None], axis=0)
    local_count = jnp.sum(lengths).astype(jnp.float32)
    group_sums, count = lax.psum((local_sums, local_count), "dp")
    adv_resp = rewards - jnp.sum(member * group_sums[None, :], axis=1) / GROUP
    adv = jnp.repeat(adv_resp, length_max)
    mask = (
        (jnp.arange(length_max, dtype=jnp.int32)[None, :] < lengths[:, None])
        .astype(jnp.float32)
        .reshape(rows)
    )
    gain_f = gain_full.astype(jnp.float32)
    inv = lax.rsqrt(
        jnp.mean(jnp.square(whole.astype(jnp.float32)), axis=1, keepdims=True) + eps_norm
    )
    normed = (whole.astype(jnp.float32) * inv * gain_f).astype(jnp.bfloat16)
    logits = lax.dot_general(
        normed, head, (((1,), (1,)), ((), ())), preferred_element_type=jnp.float32
    )
    top_local = jnp.max(logits, axis=1)
    sum_local = jnp.sum(jnp.exp(logits - top_local[:, None]), axis=1)
    local_targets = targets.reshape(rows) - vocab_start
    hits = jnp.arange(vocab_here, dtype=jnp.int32)[None, :] == local_targets[:, None]
    chosen_local = jnp.sum(jnp.where(hits, logits, 0.0), axis=1)
    stats = lax.all_gather(jnp.stack([top_local, sum_local, chosen_local]), "fsdp", axis=0)
    top = jnp.max(stats[:, 0], axis=0)
    total = jnp.sum(stats[:, 1] * jnp.exp(stats[:, 0] - top[None, :]), axis=0)
    chosen = jnp.sum(stats[:, 2], axis=0)
    lse = top + jnp.log(total)
    logp = chosen - lse
    ratio = jnp.exp(logp - old_logp.reshape(rows))
    first = ratio * adv
    second = jnp.clip(ratio, clip_low, clip_high) * adv
    policy = -jnp.minimum(first, second)
    policy = jnp.where(adv < 0, jnp.minimum(policy, -dual_bound * adv), policy)
    loss_local = jnp.sum(mask * policy)
    active = (first <= second) & jnp.logical_not((adv < 0) & (first < dual_bound * adv))
    slots_all = rows * lax.axis_size("dp")
    grad_logp = slots_all / count * mask * jnp.where(active, -ratio * adv, 0.0)
    probs = jnp.exp(logits - lse[:, None])
    dlogits = (grad_logp[:, None] * (hits.astype(jnp.float32) - probs)).astype(jnp.bfloat16)
    grad_h, grad_head_t, sums = tail(
        normed,
        dlogits,
        head,
        hidden.reshape(rows, shard_cols),
        gain.astype(jnp.float32)[None, :],
        inv,
        jnp.broadcast_to(loss_local, (8, 128)),
    )
    loss = sums[0, shard_cols] / count
    grad_gain = sums[0, :shard_cols]
    grad_hidden = grad_h.reshape(resp_here, length_max, shard_cols)
    return (loss, grad_hidden, grad_gain, grad_head_t)


def solution(mesh):
    in_specs = (
        P("dp", None, "fsdp"),
        P("fsdp"),
        P("fsdp", None),
        P("dp", None),
        P("dp"),
        P("dp", None),
        P("dp"),
        P("dp"),
    )
    out_specs = (P(), P("dp", None, "fsdp"), P("fsdp"), P("dp", "fsdp"))
    return jax.shard_map(body, mesh=mesh, in_specs=in_specs, out_specs=out_specs, check_vma=False)
```
